32 devices in a mesh: parts: 2 (over x), inner: 16 (over z, y, core).
Axes of the slice: x: 2, y: 2, z: 4, core: 2. Of those that a mesh axis runs over, the one named last changes fastest.
Arguments:
- stem_slab: bfloat16 [2, 16384, 1024], P(None, ('parts', 'inner')), parts along dimension 1, may hold values from -6 to 6
- branches: bfloat16 [3, 2, 1024, 1024], P(None, None, 'inner'), may hold values from -0.1875 to 0.1875
- column_order: int32 [3, 1024], replicated, may hold values from 0 to 1023, each once within a row
Outputs:
- result_slab: bfloat16 [2, 16384, 1024], P(None, ('parts', 'inner')), parts along dimension 1
The draws below stay inside these ranges and needn't reach their ends.
There are 2 independent parts, one for each index of `parts`. The reference program is written for one: setup_inputs(seed, part) draws one part's arguments, and reference() takes and returns one part's arrays. A program takes and returns all parts, laid end to end along the dimension named above; an argument that names none is the same for every part. Nothing has to cross between parts.
Inputs may be any that keep to these rules, and one draw needn't show every extreme that they name: Each row of column_order names every number from 0 to 1023 exactly once.
All inputs are finite; a program needn't handle non-finite values.
Results may differ from the reference program's by a relative error of at most 0.0057.
Values may be sent and summed in bfloat16 or wider, within the bound.
A program may use at most 64 MiB of HBM per device.

```python
import jax
import jax.numpy as jnp

BRANCH = 1024
ROWS_DEV = 512
STEPS = 3
ROWS = 8192
N_INNER = 16


def raised(array, key, source, target, blocks, factor):
    owner, partner = [(jnp.arange(array.shape[position]) // (array.shape[position] // blocks)).reshape([-1 if axis == position else 1 for axis in range(array.ndim)]) for position in (source, target)]
    chosen = jax.random.permutation(key, blocks)[partner]
    strong = (owner == chosen) | (owner == (partner + blocks // 2) % blocks)
    return jnp.where(strong, factor * array, array)


def block_scale(key, shape, pieces, least, top_value):
    loudness = 1.0
    for position, blocks in pieces:
        draws = jax.random.uniform(jax.random.fold_in(jax.random.fold_in(key, 6), position), (blocks,), jnp.float32, least / len(pieces), top_value / len(pieces))
        loudness = loudness * jnp.repeat(jnp.exp(draws), shape[position] // blocks).reshape((-1,) + (1,) * (len(shape) - 1 - position))
    return loudness


def noise(stream_key, extent, spread, limit, cuts=(), held_as=jnp.bfloat16):
    drawn = jax.random.normal(stream_key, extent, jnp.float32) * spread
    if len(cuts) > 0:
        drawn = block_scale(stream_key, extent, cuts, -0.22, 0.18) * drawn
    return jnp.clip(drawn, min=-limit, max=limit).astype(held_as)


def gaussian_with(own_key, extent, scale, most, cuts, heavy, kind=jnp.bfloat16):
    array = scale * jax.random.normal(own_key, extent, jnp.float32)
    if cuts:
        array = array * block_scale(own_key, extent, cuts, -0.22, 0.18)
    return jnp.clip(raised(array, jax.random.fold_in(own_key, 3), *heavy), -most, most).astype(kind)


def setup_inputs(seed: int = 0, part: int = 0) -> dict:
    key_list = jax.random.split(jax.random.key(seed), 4)
    own_keys = jax.random.split(jax.random.fold_in(key_list[3], part), 4)
    return {
        "stem_slab": noise(own_keys[0], (2, ROWS, BRANCH), 1.0, 6.0, ((1, 16),)),
        "branches": gaussian_with(key_list[1], (STEPS, 2, BRANCH, BRANCH), (2 * BRANCH) ** -0.5, 0.1875, ((2, 16),), (2, 3, 16, 2.0)),
        "column_order": jax.vmap(lambda own: jax.random.permutation(own, BRANCH))(jax.random.split(key_list[2], STEPS)).reshape((STEPS, BRANCH)).astype(jnp.int32),
    }


def contract(slab, order_row, pair):
    picked = jnp.take(slab, order_row.astype(jnp.int32), axis=2)
    real_part = jnp.dot(picked[0], pair[0], preferred_element_type=jnp.float32) - jnp.dot(picked[1], pair[1], preferred_element_type=jnp.float32)
    imag_part = jnp.dot(picked[0], pair[1], preferred_element_type=jnp.float32) + jnp.dot(picked[1], pair[0], preferred_element_type=jnp.float32)
    return jnp.stack([real_part, imag_part]).astype(jnp.bfloat16)


def swap_blocks(slab):
    width = BRANCH // N_INNER
    blocks = slab.reshape(2, N_INNER, ROWS_DEV, N_INNER, width)
    return jnp.transpose(blocks, (0, 3, 2, 1, 4)).reshape(2, N_INNER * ROWS_DEV, BRANCH)


def reference(stem_slab, branches, column_order):
    current = stem_slab
    for section_index in range(STEPS):
        if section_index > 0:
            current = swap_blocks(current)
        current = contract(current, column_order[section_index], branches[section_index])
    return current
```

```python
import functools

import jax
import jax.numpy as jnp
from jax import lax
from jax.experimental import pallas as pl
from jax.experimental.pallas import tpu as pltpu
from jax.sharding import PartitionSpec as P

CORES = 2
YS = 2
CHUNKS = 2
PACK = 16
TILE = 256
LANES = 128
F32 = jnp.float32
BF16 = jnp.bfloat16
MESH_ID = pl.DeviceIdType.MESH


def add_block(ordered, block_rows):
    real_part = jnp.dot(ordered[0], block_rows[0], preferred_element_type=F32) - jnp.dot(
        ordered[1], block_rows[1], preferred_element_type=F32
    )
    imag_part = jnp.dot(ordered[0], block_rows[1], preferred_element_type=F32) + jnp.dot(
        ordered[1], block_rows[0], preferred_element_type=F32
    )
    return jnp.stack([real_part, imag_part])


def folded(slab, order_row, branch_slice):
    ordered = jnp.take(slab, order_row, axis=2)
    summed = add_block(ordered, lax.all_gather(branch_slice, "inner", axis=1, tiled=True))
    return summed.astype(BF16)


def plain(stem_slab, branches, column_order):
    current = folded(stem_slab, column_order[0], branches[0])
    for section_index in range(1, branches.shape[0]):
        current = lax.all_to_all(current, "inner", split_axis=2, concat_axis=2, tiled=True)
        current = folded(current, column_order[section_index], branches[section_index])
    return current


def kernel(
    n, stem_hbm, branches, order, out_hbm, gathered, onehot, weights, arrived, middle, turned, swapped, result, final,
    own_sem, zs_sem, zr_sem, xs_sem, xr_sem, ys_sem, yr_sem, ds_sem, dr_sem, cs_sem, cr_sem, as_sem, ar_sem,
    here_sem, out_sem,
):
    sections = branches.shape[0]
    depth = branches.shape[2]
    total = n * depth
    columns = branches.shape[3]
    part = arrived.shape[3]
    rows = n * part
    plane = CORES * YS
    nz = n // plane
    me = lax.axis_index("inner")
    x = lax.axis_index("parts")
    z = me // plane
    low = me % plane
    y = low // CORES
    core = low % CORES
    other_low = (1 - y) * CORES + core
    x_peer = {"parts": 1 - x}
    y_peer = {"inner": z * plane + other_low}
    core_peer = {"inner": z * plane + y * CORES + (1 - core)}

    barrier = pltpu.get_barrier_semaphore()

    @pl.loop(1, n)
    def _(hop):
        pl.semaphore_signal(
            barrier, inc=1, device_id={"inner": lax.rem(me + hop, n)}, device_id_type=MESH_ID
        )

    pl.semaphore_signal(barrier, inc=1, device_id=x_peer, device_id_type=MESH_ID)
    pl.semaphore_wait(barrier, n)

    def remote(src, dst, send_sem, recv_sem, device):
        return pltpu.make_async_remote_copy(
            src_ref=src, dst_ref=dst, send_sem=send_sem, recv_sem=recv_sem,
            device_id=device, device_id_type=MESH_ID,
        )


    def block(s, zz, across, p, own=False):
        slot = zz * plane + (other_low if across else low)
        return (branches.at[s, p] if own else gathered.at[s, slot, p]), gathered.at[s, slot, p]

    def z_of(t, way):
        return z - t if way == 0 else z + t

    def z_copy(s, t, way):
        src, dst = block(s, z_of(t, way), False, x, own=t == 0)
        target = {"inner": me + plane if way == 0 else me - plane}
        return remote(src, dst, zs_sem.at[s, t, way], zr_sem.at[s, t, way], target)

    def z_sends(t, way):
        return (z - t >= 0) & (z + 1 < nz) if way == 0 else (z + t < nz) & (z >= 1)

    def z_holds(t, way):
        return z - t >= 0 if way == 0 else z + t < nz

    def x_copy(s, zz):
        src, dst = block(s, zz, False, x)
        return remote(src, dst, xs_sem.at[s, zz], xr_sem.at[s, zz], x_peer)

    def y_copy(s, zz, own=False):
        src, dst = block(s, zz, False, x, own)
        return remote(src, dst, ys_sem.at[s, zz], yr_sem.at[s, zz], y_peer)

    def diagonal_x(s, zz):
        src, dst = block(s, zz, True, x)
        return remote(src, dst, ds_sem.at[s, zz], dr_sem.at[s, zz], x_peer)

    def diagonal_y(s, zz, own=False):
        src, dst = block(s, zz, False, 1 - x, own)
        return remote(src, dst, ds_sem.at[s, zz], dr_sem.at[s, zz], y_peer)

    def core_send(s, zz, across, p, own=False):
        src, dst = block(s, zz, across, p, own)
        remote(src, dst, cs_sem.at[s], cr_sem.at[s], core_peer).start()

    def landed(s, zz, across, p, sem):
        _, dst = block(s, zz, across, p)
        remote(dst, dst, cs_sem.at[s], sem, core_peer).wait_recv()

    def begin_z(s):
        for way in (0, 1):
            @pl.when(z_sends(0, way))
            def _():
                z_copy(s, 0, way).start()

    def begin_side(s):
        y_copy(s, z, own=True).start()

        @pl.when(core == 1)
        def _():
            diagonal_y(s, z, own=True).start()

        core_send(s, z, False, x, own=True)
        core_send(s, z, False, 1 - x, own=True)
        pltpu.make_async_copy(branches.at[s], gathered.at[s, me], own_sem.at[s]).start()

    def z_step(s, t):
        for way in (0, 1):
            @pl.when(z_holds(t, way))
            def _():
                landed(s, z_of(t, way), False, x, zr_sem.at[s, t - 1, way])

                if t < nz - 1:
                    @pl.when(z_sends(t, way))
                    def _():
                        z_copy(s, t, way).start()

    def side_send(s, t):
        for way in (0, 1):
            @pl.when(z_holds(t, way))
            def _():
                zz = z_of(t, way)
                x_copy(s, zz).start()
                y_copy(s, zz).start()
                core_send(s, zz, False, x)

    def side_step(s, t):
        for way in (0,) if t == 0 else (0, 1):
            @pl.when(z_holds(t, way))
            def _():
                zz = z_of(t, way)
                landed(s, zz, True, x, yr_sem.at[s, zz])
                if t > 0:
                    diagonal_x(s, zz).start()
                else:
                    @pl.when(core == 0)
                    def _():
                        diagonal_x(s, zz).start()

                core_send(s, zz, True, x)
                if t > 0:
                    landed(s, zz, False, 1 - x, xr_sem.at[s, zz])
                    core_send(s, zz, False, 1 - x)

    def diagonal_step(s, t):
        for way in (0,) if t == 0 else (0, 1):
            @pl.when(z_holds(t, way))
            def _():
                zz = z_of(t, way)
                landed(s, zz, True, 1 - x, dr_sem.at[s, zz])
                core_send(s, zz, True, 1 - x)

    def finish(s):
        half = gathered.at[s, pl.ds(0, n // CORES)]
        remote(half, half, cs_sem.at[s], cr_sem.at[s], core_peer).wait_recv()
        pltpu.make_async_copy(branches.at[s], gathered.at[s, me], own_sem.at[s]).wait()


    half_n = n // 2
    own_base = (z // (nz // 2)) * half_n
    both = pl.ds(1, 2)

    def stem_at(c, t):
        return stem_hbm.at[:, t, pl.ds(c * part, part)]

    def out_at(t, c):
        return out_hbm.at[:, t, pl.ds(c * part, part)]

    def row_source(e, t):
        return stem_at(e, t) if e < CHUNKS else turned.at[0, both, t] if e == CHUNKS else result.at[:, t]

    def row_target(e, t):
        return arrived.at[e, both, t] if e < CHUNKS else swapped.at[both, t] if e == CHUNKS else out_at(t, 1)

    def row_send(e, t):
        remote(row_source(e, t), row_target(e, me), as_sem.at[e], ar_sem.at[e], {"inner": t}).start()

    def send_far(e):
        for h in range(nz // 2):
            there = jnp.where(z < nz // 2, nz // 2 + h, nz // 2 - 1 - h) * plane

            @pl.loop(0, plane)
            def _(i):
                row_send(e, there + lax.rem(me + i, plane))

    def send_near(e):
        @pl.loop(1, half_n)
        def _(i):
            row_send(e, own_base + lax.rem(me + i, half_n))

    def rows_of(e):
        if e < CHUNKS:
            return arrived.at[e, both, pl.ds(0, n - 1)]
        if e == CHUNKS:
            return swapped.at[both, pl.ds(0, n - 1)]
        return out_hbm.at[:, pl.ds(0, n - 1), pl.ds(part, part)]

    def row_wait(e):
        part_rows = rows_of(e)
        return remote(part_rows, part_rows, as_sem.at[e], ar_sem.at[e], core_peer)

    def stem_here(c):
        return pltpu.make_async_copy(stem_at(c, me), arrived.at[c, both, me], here_sem.at[c])

    def build_onehot(s):
        @pl.loop(0, total // LANES)
        def _(i):
            span = pl.ds(pl.multiple_of(i * LANES, LANES), LANES)
            target = lax.broadcasted_iota(jnp.int32, (LANES, total), 0) + i * LANES
            onehot[span, :] = jnp.where(order[s : s + 1, :] == target, 1.0, 0.0).astype(BF16)

    def prepare(s, first=0, last=None):
        @pl.loop(first, columns // TILE if last is None else last)
        def _(j):
            cols = pl.ds(pl.multiple_of(j * TILE, TILE), TILE)
            for p in range(2):
                block_rows = gathered[s, :, p, :, cols].reshape(total, TILE)
                for i in range(total // TILE):
                    span = slice(i * TILE, (i + 1) * TILE)
                    weights[s, p, span, cols] = jnp.dot(
                        onehot[span, :], block_rows, preferred_element_type=F32
                    ).astype(BF16)

    def negate(left):
        @pl.loop(0, n)
        def _(g):
            left[0, g] = -left[2, g]

    def multiply(s, left, store):
        @pl.loop(0, columns // TILE)
        def _(j):
            cols = pl.ds(pl.multiple_of(j * TILE, TILE), TILE)
            straight = left[1:3].reshape(2 * rows, total)
            crossed = left[0:2].reshape(2 * rows, total)
            product = jnp.dot(straight, weights[s, 0, :, cols], preferred_element_type=F32) + jnp.dot(
                crossed, weights[s, 1, :, cols], preferred_element_type=F32
            )
            store(j, cols, product[:rows], product[rows:])

    low_half = lax.broadcasted_iota(jnp.int32, (part, LANES), 1) < LANES // 2

    def turn(into):
        def store(j, cols, real, imag):
            for p, value in ((1, real), (2, imag)):
                for t in range(TILE // LANES):
                    d = (j * (TILE // LANES) + t) * 2
                    lanes = slice(t * LANES, (t + 1) * LANES)
                    for h in range(n // 2):
                        first = value[2 * h * part : (2 * h + 1) * part, lanes]
                        second = value[(2 * h + 1) * part : (2 * h + 2) * part, lanes]
                        mixed = pltpu.roll(jnp.where(low_half, second, first), LANES // 2, 1)
                        at = slice(h * LANES, (h + 1) * LANES)
                        for b, block_value in ((d, jnp.where(low_half, first, mixed)), (d + 1, jnp.where(low_half, mixed, second))):
                            into[p, b, :, at] = block_value.astype(BF16)
                            if p == 2:
                                into[0, b, :, at] = (-block_value).astype(BF16)
        return store

    def keep(into):
        def store(j, cols, real, imag):
            into[0, :, :, cols] = real.astype(BF16).reshape(n, part, TILE)
            into[1, :, :, cols] = imag.astype(BF16).reshape(n, part, TILE)
        return store

    tiles = columns // TILE
    begin_z(0)
    begin_z(1)
    begin_side(0)
    begin_side(1)
    for c in range(CHUNKS):
        stem_here(c).start()
    build_onehot(0)
    z_step(0, 1)
    side_send(0, 1)
    begin_z(2)
    z_step(1, 1)
    side_send(1, 1)
    side_step(0, 0)
    z_step(0, 2)
    side_send(0, 2)
    z_step(2, 1)
    send_far(0)
    z_step(1, 2)
    side_send(1, 2)
    side_step(0, 1)
    z_step(0, 3)
    side_send(0, 3)
    side_step(1, 0)
    side_step(0, 2)
    diagonal_step(0, 0)
    z_step(1, 3)
    side_send(1, 3)
    side_step(1, 1)
    send_near(0)
    z_step(2, 2)
    side_step(0, 3)
    diagonal_step(0, 1)
    side_step(1, 2)
    send_far(1)
    diagonal_step(0, 2)
    side_step(1, 3)
    diagonal_step(0, 3)
    send_near(1)
    finish(0)
    prepare(0, 0, tiles // 2)
    diagonal_step(1, 0)
    z_step(2, 3)
    diagonal_step(1, 1)
    prepare(0, tiles // 2, tiles)
    diagonal_step(1, 2)
    diagonal_step(1, 3)
    begin_side(2)
    for t in range(1, nz):
        side_send(2, t)
    build_onehot(1)
    stem_here(0).wait()
    row_wait(0).wait_recv()
    negate(arrived.at[0])
    multiply(0, arrived.at[0], turn(middle))
    finish(1)
    prepare(1)
    multiply(1, middle, turn(turned.at[0]))
    swapped[both, me] = turned[0, both, me]
    send_far(2)
    send_near(2)
    build_onehot(2)
    side_step(2, 0)
    side_step(2, 1)
    stem_here(1).wait()
    row_wait(1).wait_recv()
    negate(arrived.at[1])
    multiply(0, arrived.at[1], turn(middle))
    for t in range(2, nz):
        side_step(2, t)
    multiply(1, middle, turn(turned.at[1]))
    for t in range(nz):
        diagonal_step(2, t)
    finish(2)
    prepare(2)
    multiply(2, turned.at[1], keep(result))
    send_far(3)
    send_near(3)
    own_out = pltpu.make_async_copy(result.at[:, me], out_at(me, 1), here_sem.at[0])
    own_out.start()
    row_wait(2).wait_recv()
    negate(swapped)
    multiply(2, swapped, keep(final))
    first_out = pltpu.make_async_copy(final, out_hbm.at[:, :, pl.ds(0, part)], out_sem)
    first_out.start()

    for s in range(sections):
        for t in range(nz - 1):
            for way in (0, 1):
                @pl.when(z_sends(t, way))
                def _():
                    z_copy(s, t, way).wait_send()
        for zz in range(nz):
            @pl.when(z != zz)
            def _():
                x_copy(s, zz).wait_send()

            y_copy(s, zz).wait_send()
            diagonal_y(s, zz).wait_send()
        half = gathered.at[s, pl.ds(0, n // CORES)]
        remote(half, half, cs_sem.at[s], cr_sem.at[s], core_peer).wait_send()
    for e in range(2 * CHUNKS):
        row_wait(e).wait_send()
    own_out.wait()
    first_out.wait()
    row_wait(3).wait_recv()


def fused(n, stem_slab, branches, column_order):
    sections, _, depth, columns = branches.shape
    share = stem_slab.shape[1] // n
    part = share // CHUNKS
    nz = n // (CORES * YS)
    total = n * depth
    dma = pltpu.SemaphoreType.DMA
    stem = stem_slab.reshape(2, n, share, columns)
    result = pl.pallas_call(
        functools.partial(kernel, n),
        out_shape=jax.ShapeDtypeStruct(stem.shape, BF16),
        in_specs=[pl.BlockSpec(memory_space=pl.ANY)] + [pl.BlockSpec(memory_space=pltpu.VMEM)] * 2,
        out_specs=pl.BlockSpec(memory_space=pl.ANY),
        scratch_shapes=[
            pltpu.VMEM((sections, n, 2, depth, columns), BF16),
            pltpu.VMEM((total, total), BF16),
            pltpu.VMEM((sections, 2, total, columns), BF16),
            pltpu.VMEM((CHUNKS, 3, n, part, columns), BF16),
            pltpu.VMEM((3, n, part, columns), BF16),
            pltpu.VMEM((CHUNKS, 3, n, part, columns), BF16),
            pltpu.VMEM((3, n, part, columns), BF16),
            pltpu.VMEM((2, n, part, columns), BF16),
            pltpu.VMEM((2, n, part, columns), BF16),
            dma((sections,)),
            dma((sections, nz, 2)),
            dma((sections, nz, 2)),
            *[dma((sections, nz))] * 6,
            dma((sections,)),
            dma((sections,)),
            dma((2 * CHUNKS,)),
            dma((2 * CHUNKS,)),
            dma((CHUNKS,)),
            dma,
        ],
        compiler_params=pltpu.CompilerParams(
            collective_id=0, has_side_effects=True, vmem_limit_bytes=60 * 2**20
        ),
    )(stem, branches, column_order)
    return result.reshape(stem_slab.shape)


def solution(mesh):
    n = mesh.shape["inner"]

    def local(stem_slab, branches, column_order):
        columns = branches.shape[3]
        fits = mesh.shape["parts"] == 2 and 2 * (columns // n) == LANES and n == 4 * CORES * YS
        even = stem_slab.shape[1] == n * CHUNKS * PACK and columns % TILE == 0
        if fits and even and branches.shape[0] == 3 and columns == n * branches.shape[2]:
            return fused(n, stem_slab, branches, column_order)
        return plain(stem_slab, branches, column_order)

    in_specs = (P(None, ("parts", "inner"), None), P(None, None, "inner", None), P())
    out_specs = P(None, ("parts", "inner"), None)
    return jax.shard_map(local, mesh=mesh, in_specs=in_specs, out_specs=out_specs, check_vma=False)
```

```python
import functools

import jax
import jax.numpy as jnp
from jax import lax
from jax.experimental import pallas as pl
from jax.experimental.pallas import tpu as pltpu
from jax.sharding import PartitionSpec as P

CORES = 2
YS = 2
CHUNKS = 2
PACK = 16
TILE = 256
LANES = 128
F32 = jnp.float32
BF16 = jnp.bfloat16
MESH_ID = pl.DeviceIdType.MESH


def add_block(ordered, block_rows):
    real_part = jnp.dot(ordered[0], block_rows[0], preferred_element_type=F32) - jnp.dot(
        ordered[1], block_rows[1], preferred_element_type=F32
    )
    imag_part = jnp.dot(ordered[0], block_rows[1], preferred_element_type=F32) + jnp.dot(
        ordered[1], block_rows[0], preferred_element_type=F32
    )
    return jnp.stack([real_part, imag_part])


def folded(slab, order_row, branch_slice):
    ordered = jnp.take(slab, order_row, axis=2)
    summed = add_block(ordered, lax.all_gather(branch_slice, "inner", axis=1, tiled=True))
    return summed.astype(BF16)


def plain(stem_slab, branches, column_order):
    current = folded(stem_slab, column_order[0], branches[0])
    for section_index in range(1, branches.shape[0]):
        current = lax.all_to_all(current, "inner", split_axis=2, concat_axis=2, tiled=True)
        current = folded(current, column_order[section_index], branches[section_index])
    return current


def kernel(
    n, stem_hbm, branches_hbm, order_hbm, out_hbm, branches, order, gathered, onehot, weights, arrived, middle, turned, swapped, result, final,
    own_sem, zs_sem, zr_sem, xs_sem, xr_sem, ys_sem, yr_sem, ds_sem, dr_sem, cs_sem, cr_sem, as_sem, ar_sem,
    here_sem, out_sem, in_sem,
):
    sections = branches.shape[0]
    depth = branches.shape[2]
    total = n * depth
    columns = branches.shape[3]
    part = arrived.shape[3]
    rows = n * part
    plane = CORES * YS
    nz = n // plane
    me = lax.axis_index("inner")
    x = lax.axis_index("parts")
    z = me // plane
    low = me % plane
    y = low // CORES
    core = low % CORES
    other_low = (1 - y) * CORES + core
    x_peer = {"parts": 1 - x}
    y_peer = {"inner": z * plane + other_low}
    core_peer = {"inner": z * plane + y * CORES + (1 - core)}

    branches_in = pltpu.make_async_copy(branches_hbm, branches, in_sem.at[0])
    branches_in.start()
    order_in = pltpu.make_async_copy(order_hbm, order, in_sem.at[1])
    order_in.start()
    stem_in = [
        pltpu.make_async_copy(
            stem_hbm.at[:, me, pl.ds(c * part, part)], arrived.at[c, pl.ds(1, 2), me], here_sem.at[c]
        )
        for c in range(CHUNKS)
    ]
    for copy in stem_in:
        copy.start()
    barrier = pltpu.get_barrier_semaphore()

    @pl.loop(1, n)
    def _(hop):
        pl.semaphore_signal(
            barrier, inc=1, device_id={"inner": lax.rem(me + hop, n)}, device_id_type=MESH_ID
        )

    pl.semaphore_signal(barrier, inc=1, device_id=x_peer, device_id_type=MESH_ID)
    pl.semaphore_wait(barrier, n)

    def remote(src, dst, send_sem, recv_sem, device):
        return pltpu.make_async_remote_copy(
            src_ref=src, dst_ref=dst, send_sem=send_sem, recv_sem=recv_sem,
            device_id=device, device_id_type=MESH_ID,
        )


    def block(s, zz, across, p, own=False):
        slot = zz * plane + (other_low if across else low)
        return (branches.at[s, p] if own else gathered.at[s, slot, p]), gathered.at[s, slot, p]

    def z_of(t, way):
        return z - t if way == 0 else z + t

    def z_copy(s, t, way):
        src, dst = block(s, z_of(t, way), False, x, own=t == 0)
        target = {"inner": me + plane if way == 0 else me - plane}
        return remote(src, dst, zs_sem.at[s, t, way], zr_sem.at[s, t, way], target)

    def z_sends(t, way):
        return (z - t >= 0) & (z + 1 < nz) if way == 0 else (z + t < nz) & (z >= 1)

    def z_holds(t, way):
        return z - t >= 0 if way == 0 else z + t < nz

    def x_copy(s, zz):
        src, dst = block(s, zz, False, x)
        return remote(src, dst, xs_sem.at[s, zz], xr_sem.at[s, zz], x_peer)

    def y_copy(s, zz, own=False):
        src, dst = block(s, zz, False, x, own)
        return remote(src, dst, ys_sem.at[s, zz], yr_sem.at[s, zz], y_peer)

    def diagonal_x(s, zz):
        src, dst = block(s, zz, True, x)
        return remote(src, dst, ds_sem.at[s, zz], dr_sem.at[s, zz], x_peer)

    def diagonal_y(s, zz, own=False):
        src, dst = block(s, zz, False, 1 - x, own)
        return remote(src, dst, ds_sem.at[s, zz], dr_sem.at[s, zz], y_peer)

    def core_send(s, zz, across, p, own=False):
        src, dst = block(s, zz, across, p, own)
        remote(src, dst, cs_sem.at[s], cr_sem.at[s], core_peer).start()

    def landed(s, zz, across, p, sem):
        _, dst = block(s, zz, across, p)
        remote(dst, dst, cs_sem.at[s], sem, core_peer).wait_recv()

    def begin_z(s):
        for way in (0, 1):
            @pl.when(z_sends(0, way))
            def _():
                z_copy(s, 0, way).start()

    def begin_side(s):
        y_copy(s, z, own=True).start()

        @pl.when(core == 1)
        def _():
            diagonal_y(s, z, own=True).start()

        core_send(s, z, False, x, own=True)
        core_send(s, z, False, 1 - x, own=True)
        pltpu.make_async_copy(branches.at[s], gathered.at[s, me], own_sem.at[s]).start()

    def z_step(s, t):
        for way in (0, 1):
            @pl.when(z_holds(t, way))
            def _():
                landed(s, z_of(t, way), False, x, zr_sem.at[s, t - 1, way])

                if t < nz - 1:
                    @pl.when(z_sends(t, way))
                    def _():
                        z_copy(s, t, way).start()

    def side_send(s, t):
        for way in (0, 1):
            @pl.when(z_holds(t, way))
            def _():
                zz = z_of(t, way)
                x_copy(s, zz).start()
                y_copy(s, zz).start()
                core_send(s, zz, False, x)

    def side_step(s, t):
        for way in (0,) if t == 0 else (0, 1):
            @pl.when(z_holds(t, way))
            def _():
                zz = z_of(t, way)
                landed(s, zz, True, x, yr_sem.at[s, zz])
                if t > 0:
                    diagonal_x(s, zz).start()
                else:
                    @pl.when(core == 0)
                    def _():
                        diagonal_x(s, zz).start()

                core_send(s, zz, True, x)
                if t > 0:
                    landed(s, zz, False, 1 - x, xr_sem.at[s, zz])
                    core_send(s, zz, False, 1 - x)

    def diagonal_step(s, t):
        for way in (0,) if t == 0 else (0, 1):
            @pl.when(z_holds(t, way))
            def _():
                zz = z_of(t, way)
                landed(s, zz, True, 1 - x, dr_sem.at[s, zz])
                core_send(s, zz, True, 1 - x)

    def finish(s):
        half = gathered.at[s, pl.ds(0, n // CORES)]
        remote(half, half, cs_sem.at[s], cr_sem.at[s], core_peer).wait_recv()
        pltpu.make_async_copy(branches.at[s], gathered.at[s, me], own_sem.at[s]).wait()


    half_n = n // 2
    own_base = (z // (nz // 2)) * half_n
    both = pl.ds(1, 2)

    def stem_at(c, t):
        return stem_hbm.at[:, t, pl.ds(c * part, part)]

    def out_at(t, c):
        return out_hbm.at[:, t, pl.ds(c * part, part)]

    def row_source(e, t):
        return stem_at(e, t) if e < CHUNKS else turned.at[0, both, t] if e == CHUNKS else result.at[:, t]

    def row_target(e, t):
        return arrived.at[e, both, t] if e < CHUNKS else swapped.at[both, t] if e == CHUNKS else out_at(t, 1)

    def row_send(e, t):
        remote(row_source(e, t), row_target(e, me), as_sem.at[e], ar_sem.at[e], {"inner": t}).start()

    def send_far(e, planes):
        for h in planes:
            there = jnp.where(z < nz // 2, nz // 2 + h, nz // 2 - 1 - h) * plane

            @pl.loop(0, plane)
            def _(i):
                row_send(e, there + lax.rem(me + i, plane))

    def send_near(e):
        @pl.loop(1, half_n)
        def _(i):
            row_send(e, own_base + lax.rem(me + i, half_n))

    def rows_of(e):
        if e < CHUNKS:
            return arrived.at[e, both, pl.ds(0, n - 1)]
        if e == CHUNKS:
            return swapped.at[both, pl.ds(0, n - 1)]
        return out_hbm.at[:, pl.ds(0, n - 1), pl.ds(part, part)]

    def row_wait(e):
        part_rows = rows_of(e)
        return remote(part_rows, part_rows, as_sem.at[e], ar_sem.at[e], core_peer)

    def build_onehot(s):
        @pl.loop(0, total // LANES)
        def _(i):
            span = pl.ds(pl.multiple_of(i * LANES, LANES), LANES)
            target = lax.broadcasted_iota(jnp.int32, (LANES, total), 0) + i * LANES
            onehot[span, :] = jnp.where(order[s : s + 1, :] == target, 1.0, 0.0).astype(BF16)

    def prepare(s, first=0, last=None):
        @pl.loop(first, columns // TILE if last is None else last)
        def _(j):
            cols = pl.ds(pl.multiple_of(j * TILE, TILE), TILE)
            for p in range(2):
                block_rows = gathered[s, :, p, :, cols].reshape(total, TILE)
                for i in range(total // TILE):
                    span = slice(i * TILE, (i + 1) * TILE)
                    weights[s, p, span, cols] = jnp.dot(
                        onehot[span, :], block_rows, preferred_element_type=F32
                    ).astype(BF16)

    def negate(left):
        @pl.loop(0, n)
        def _(g):
            left[0, g] = -left[2, g]

    def multiply(s, left, store):
        @pl.loop(0, columns // TILE)
        def _(j):
            cols = pl.ds(pl.multiple_of(j * TILE, TILE), TILE)
            straight = left[1:3].reshape(2 * rows, total)
            crossed = left[0:2].reshape(2 * rows, total)
            product = jnp.dot(straight, weights[s, 0, :, cols], preferred_element_type=F32) + jnp.dot(
                crossed, weights[s, 1, :, cols], preferred_element_type=F32
            )
            store(j, cols, product[:rows], product[rows:])

    low_half = lax.broadcasted_iota(jnp.int32, (part, LANES), 1) < LANES // 2

    def turn(into):
        def store(j, cols, real, imag):
            for p, value in ((1, real), (2, imag)):
                for t in range(TILE // LANES):
                    d = (j * (TILE // LANES) + t) * 2
                    lanes = slice(t * LANES, (t + 1) * LANES)
                    for h in range(n // 2):
                        first = value[2 * h * part : (2 * h + 1) * part, lanes]
                        second = value[(2 * h + 1) * part : (2 * h + 2) * part, lanes]
                        mixed = pltpu.roll(jnp.where(low_half, second, first), LANES // 2, 1)
                        at = slice(h * LANES, (h + 1) * LANES)
                        for b, block_value in ((d, jnp.where(low_half, first, mixed)), (d + 1, jnp.where(low_half, mixed, second))):
                            into[p, b, :, at] = block_value.astype(BF16)
                            if p == 2:
                                into[0, b, :, at] = (-block_value).astype(BF16)
        return store

    def keep(into):
        def store(j, cols, real, imag):
            into[0, :, :, cols] = real.astype(BF16).reshape(n, part, TILE)
            into[1, :, :, cols] = imag.astype(BF16).reshape(n, part, TILE)
        return store

    tiles = columns // TILE
    outward = tuple(range(nz // 2))
    branches_in.wait()
    begin_z(0)
    begin_z(1)
    begin_side(0)
    begin_side(1)
    order_in.wait()
    build_onehot(0)
    z_step(0, 1)
    side_send(0, 1)
    begin_z(2)
    z_step(1, 1)
    side_send(1, 1)
    side_step(0, 0)
    z_step(0, 2)
    side_send(0, 2)
    z_step(2, 1)
    z_step(1, 2)
    side_send(1, 2)
    send_far(0, outward)
    side_step(0, 1)
    z_step(0, 3)
    side_send(0, 3)
    side_step(1, 0)
    side_step(0, 2)
    diagonal_step(0, 0)
    z_step(1, 3)
    side_send(1, 3)
    side_step(1, 1)
    send_near(0)
    z_step(2, 2)
    side_step(0, 3)
    diagonal_step(0, 1)
    side_step(1, 2)
    diagonal_step(0, 2)
    send_far(1, outward[::-1])
    side_step(1, 3)
    diagonal_step(0, 3)
    send_near(1)
    begin_side(2)
    side_send(2, 1)
    side_send(2, 2)
    finish(0)
    prepare(0, 0, tiles // 2)
    diagonal_step(1, 0)
    diagonal_step(1, 1)
    prepare(0, tiles // 2, tiles)
    diagonal_step(1, 2)
    diagonal_step(1, 3)
    build_onehot(1)
    finish(1)
    prepare(1, 0, tiles // 2)
    side_step(2, 0)
    z_step(2, 3)
    side_send(2, 3)
    prepare(1, tiles // 2, tiles)
    stem_in[0].wait()
    row_wait(0).wait_recv()
    negate(arrived.at[0])
    multiply(0, arrived.at[0], turn(middle))
    diagonal_step(2, 0)
    multiply(1, middle, turn(turned.at[0]))
    swapped[both, me] = turned[0, both, me]
    send_far(2, outward[:1])
    build_onehot(2)
    side_step(2, 1)
    stem_in[1].wait()
    row_wait(1).wait_recv()
    send_far(2, outward[1:])
    send_near(2)
    side_step(2, 2)
    negate(arrived.at[1])
    multiply(0, arrived.at[1], turn(middle))
    side_step(2, 3)
    diagonal_step(2, 1)
    multiply(1, middle, turn(turned.at[1]))
    diagonal_step(2, 2)
    diagonal_step(2, 3)
    finish(2)
    prepare(2)
    multiply(2, turned.at[1], keep(result))
    send_far(3, outward[::-1])
    send_near(3)
    own_out = pltpu.make_async_copy(result.at[:, me], out_at(me, 1), here_sem.at[0])
    own_out.start()
    row_wait(2).wait_recv()
    negate(swapped)
    multiply(2, swapped, keep(final))
    first_out = pltpu.make_async_copy(final, out_hbm.at[:, :, pl.ds(0, part)], out_sem)
    first_out.start()

    for s in range(sections):
        for t in range(nz - 1):
            for way in (0, 1):
                @pl.when(z_sends(t, way))
                def _():
                    z_copy(s, t, way).wait_send()
        for zz in range(nz):
            @pl.when(z != zz)
            def _():
                x_copy(s, zz).wait_send()

            y_copy(s, zz).wait_send()
            diagonal_y(s, zz).wait_send()
        half = gathered.at[s, pl.ds(0, n // CORES)]
        remote(half, half, cs_sem.at[s], cr_sem.at[s], core_peer).wait_send()
    for e in range(2 * CHUNKS):
        row_wait(e).wait_send()
    own_out.wait()
    first_out.wait()
    row_wait(3).wait_recv()


def fused(n, stem_slab, branches, column_order):
    sections, _, depth, columns = branches.shape
    share = stem_slab.shape[1] // n
    part = share // CHUNKS
    nz = n // (CORES * YS)
    total = n * depth
    dma = pltpu.SemaphoreType.DMA
    stem = stem_slab.reshape(2, n, share, columns)
    result = pl.pallas_call(
        functools.partial(kernel, n),
        out_shape=pltpu.VMEM(stem.shape, BF16),
        in_specs=[pl.BlockSpec(memory_space=pltpu.HBM)] * 3,
        out_specs=pl.BlockSpec(memory_space=pl.ANY),
        scratch_shapes=[
            pltpu.VMEM(branches.shape, BF16),
            pltpu.VMEM(column_order.shape, jnp.int32),
            pltpu.VMEM((sections, n, 2, depth, columns), BF16),
            pltpu.VMEM((total, total), BF16),
            pltpu.VMEM((sections, 2, total, columns), BF16),
            pltpu.VMEM((CHUNKS, 3, n, part, columns), BF16),
            pltpu.VMEM((3, n, part, columns), BF16),
            pltpu.VMEM((CHUNKS, 3, n, part, columns), BF16),
            pltpu.VMEM((3, n, part, columns), BF16),
            pltpu.VMEM((2, n, part, columns), BF16),
            pltpu.VMEM((2, n, part, columns), BF16),
            dma((sections,)),
            dma((sections, nz, 2)),
            dma((sections, nz, 2)),
            *[dma((sections, nz))] * 6,
            dma((sections,)),
            dma((sections,)),
            dma((2 * CHUNKS,)),
            dma((2 * CHUNKS,)),
            dma((CHUNKS,)),
            dma,
            dma((2,)),
        ],
        compiler_params=pltpu.CompilerParams(
            collective_id=0, has_side_effects=True, vmem_limit_bytes=61 * 2**20
        ),
    )(stem, branches, column_order)
    return result.reshape(stem_slab.shape)


def solution(mesh):
    n = mesh.shape["inner"]

    def local(stem_slab, branches, column_order):
        columns = branches.shape[3]
        fits = mesh.shape["parts"] == 2 and 2 * (columns // n) == LANES and n == 4 * CORES * YS
        even = stem_slab.shape[1] == n * CHUNKS * PACK and columns % TILE == 0
        if fits and even and branches.shape[0] == 3 and columns == n * branches.shape[2]:
            return fused(n, stem_slab, branches, column_order)
        return plain(stem_slab, branches, column_order)

    in_specs = (P(None, ("parts", "inner"), None), P(None, None, "inner", None), P())
    out_specs = P(None, ("parts", "inner"), None)
    return jax.shard_map(local, mesh=mesh, in_specs=in_specs, out_specs=out_specs, check_vma=False)
```

```python
import functools

import jax
import jax.numpy as jnp
from jax import lax
from jax.experimental import pallas as pl
from jax.experimental.pallas import tpu as pltpu
from jax.sharding import PartitionSpec as P

CORES = 2
YS = 2
CHUNKS = 2
PACK = 16
TILE = 256
LANES = 128
F32 = jnp.float32
BF16 = jnp.bfloat16
MESH_ID = pl.DeviceIdType.MESH


def add_block(ordered, block_rows):
    real_part = jnp.dot(ordered[0], block_rows[0], preferred_element_type=F32) - jnp.dot(
        ordered[1], block_rows[1], preferred_element_type=F32
    )
    imag_part = jnp.dot(ordered[0], block_rows[1], preferred_element_type=F32) + jnp.dot(
        ordered[1], block_rows[0], preferred_element_type=F32
    )
    return jnp.stack([real_part, imag_part])


def folded(slab, order_row, branch_slice):
    ordered = jnp.take(slab, order_row, axis=2)
    summed = add_block(ordered, lax.all_gather(branch_slice, "inner", axis=1, tiled=True))
    return summed.astype(BF16)


def plain(stem_slab, branches, column_order):
    current = folded(stem_slab, column_order[0], branches[0])
    for section_index in range(1, branches.shape[0]):
        current = lax.all_to_all(current, "inner", split_axis=2, concat_axis=2, tiled=True)
        current = folded(current, column_order[section_index], branches[section_index])
    return current


def kernel(
    n, stem_hbm, branches_hbm, order_hbm, out_hbm, branches, order, gathered, onehot, weights, arrived, middle, turned, swapped, result, final,
    own_sem, zs_sem, zr_sem, xs_sem, xr_sem, ys_sem, yr_sem, ds_sem, dr_sem, cs_sem, cr_sem, as_sem, ar_sem,
    here_sem, out_sem, in_sem, order_sem, meet_sem,
):
    sections = branches.shape[0]
    depth = branches.shape[2]
    total = n * depth
    columns = branches.shape[3]
    part = arrived.shape[3]
    rows = n * part
    plane = CORES * YS
    nz = n // plane
    me = lax.axis_index("inner")
    x = lax.axis_index("parts")
    z = me // plane
    low = me % plane
    y = low // CORES
    core = low % CORES
    other_low = (1 - y) * CORES + core
    x_peer = {"parts": 1 - x}
    y_peer = {"inner": z * plane + other_low}
    core_peer = {"inner": z * plane + y * CORES + (1 - core)}

    branches_in = [
        pltpu.make_async_copy(branches_hbm.at[s], branches.at[s], in_sem.at[s]) for s in range(sections)
    ]
    for copy in branches_in:
        copy.start()
    order_in = pltpu.make_async_copy(order_hbm, order, order_sem)
    order_in.start()
    stem_in = [
        pltpu.make_async_copy(
            stem_hbm.at[:, me, pl.ds(c * part, part)], arrived.at[c, pl.ds(1, 2), me], here_sem.at[c]
        )
        for c in range(CHUNKS)
    ]
    for copy in stem_in:
        copy.start()
    barrier = pltpu.get_barrier_semaphore()


    def greet(sem):
        for peer in (y_peer, core_peer):
            pl.semaphore_signal(sem, inc=1, device_id=peer, device_id_type=MESH_ID)

        @pl.when(z + 1 < nz)
        def _():
            pl.semaphore_signal(sem, inc=1, device_id={"inner": me + plane}, device_id_type=MESH_ID)

        @pl.when(z >= 1)
        def _():
            pl.semaphore_signal(sem, inc=1, device_id={"inner": me - plane}, device_id_type=MESH_ID)

    greeted = 2 + jnp.where(z + 1 < nz, 1, 0) + jnp.where(z >= 1, 1, 0)

    def meet(i):
        pl.semaphore_wait(meet_sem.at[i], greeted)
        if i + 1 < nz:
            greet(meet_sem.at[i + 1])

    pl.semaphore_signal(barrier, inc=1, device_id=x_peer, device_id_type=MESH_ID)
    greet(barrier)
    pl.semaphore_wait(barrier, greeted + 1)

    def remote(src, dst, send_sem, recv_sem, device):
        return pltpu.make_async_remote_copy(
            src_ref=src, dst_ref=dst, send_sem=send_sem, recv_sem=recv_sem,
            device_id=device, device_id_type=MESH_ID,
        )


    def block(s, zz, across, p, own=False):
        slot = zz * plane + (other_low if across else low)
        return (branches.at[s, p] if own else gathered.at[s, slot, p]), gathered.at[s, slot, p]

    def z_of(t, way):
        return z - t if way == 0 else z + t

    def z_copy(s, t, way):
        src, dst = block(s, z_of(t, way), False, x, own=t == 0)
        target = {"inner": me + plane if way == 0 else me - plane}
        return remote(src, dst, zs_sem.at[s, t, way], zr_sem.at[s, t, way], target)

    def z_sends(t, way):
        return (z - t >= 0) & (z + 1 < nz) if way == 0 else (z + t < nz) & (z >= 1)

    def z_holds(t, way):
        return z - t >= 0 if way == 0 else z + t < nz

    def x_copy(s, zz):
        src, dst = block(s, zz, False, x)
        return remote(src, dst, xs_sem.at[s, zz], xr_sem.at[s, zz], x_peer)

    def y_copy(s, zz, own=False):
        src, dst = block(s, zz, False, x, own)
        return remote(src, dst, ys_sem.at[s, zz], yr_sem.at[s, zz], y_peer)

    def diagonal_x(s, zz):
        src, dst = block(s, zz, True, x)
        return remote(src, dst, ds_sem.at[s, zz], dr_sem.at[s, zz], x_peer)

    def diagonal_y(s, zz, own=False):
        src, dst = block(s, zz, False, 1 - x, own)
        return remote(src, dst, ds_sem.at[s, zz], dr_sem.at[s, zz], y_peer)

    def core_send(s, zz, across, p, own=False):
        src, dst = block(s, zz, across, p, own)
        remote(src, dst, cs_sem.at[s], cr_sem.at[s], core_peer).start()

    def landed(s, zz, across, p, sem):
        _, dst = block(s, zz, across, p)
        remote(dst, dst, cs_sem.at[s], sem, core_peer).wait_recv()

    def begin_z(s):
        for way in (0, 1):
            @pl.when(z_sends(0, way))
            def _():
                z_copy(s, 0, way).start()

    def begin_side(s):
        y_copy(s, z, own=True).start()

        @pl.when(core == 1)
        def _():
            diagonal_y(s, z, own=True).start()

        core_send(s, z, False, x, own=True)
        core_send(s, z, False, 1 - x, own=True)
        pltpu.make_async_copy(branches.at[s], gathered.at[s, me], own_sem.at[s]).start()

    def z_step(s, t):
        for way in (0, 1):
            @pl.when(z_holds(t, way))
            def _():
                landed(s, z_of(t, way), False, x, zr_sem.at[s, t - 1, way])

                if t < nz - 1:
                    @pl.when(z_sends(t, way))
                    def _():
                        z_copy(s, t, way).start()

    def side_send(s, t):
        for way in (0, 1):
            @pl.when(z_holds(t, way))
            def _():
                zz = z_of(t, way)
                x_copy(s, zz).start()
                y_copy(s, zz).start()
                core_send(s, zz, False, x)

    def side_step(s, t):
        for way in (0,) if t == 0 else (0, 1):
            @pl.when(z_holds(t, way))
            def _():
                zz = z_of(t, way)
                landed(s, zz, True, x, yr_sem.at[s, zz])
                if t > 0:
                    diagonal_x(s, zz).start()
                else:
                    @pl.when(core == 0)
                    def _():
                        diagonal_x(s, zz).start()

                core_send(s, zz, True, x)
                if t > 0:
                    landed(s, zz, False, 1 - x, xr_sem.at[s, zz])
                    core_send(s, zz, False, 1 - x)

    def diagonal_step(s, t):
        for way in (0,) if t == 0 else (0, 1):
            @pl.when(z_holds(t, way))
            def _():
                zz = z_of(t, way)
                landed(s, zz, True, 1 - x, dr_sem.at[s, zz])
                core_send(s, zz, True, 1 - x)

    def finish(s):
        half = gathered.at[s, pl.ds(0, n // CORES)]
        remote(half, half, cs_sem.at[s], cr_sem.at[s], core_peer).wait_recv()
        pltpu.make_async_copy(branches.at[s], gathered.at[s, me], own_sem.at[s]).wait()


    half_n = n // 2
    own_base = (z // (nz // 2)) * half_n
    both = pl.ds(1, 2)

    def stem_at(c, t):
        return stem_hbm.at[:, t, pl.ds(c * part, part)]

    def out_at(t, c):
        return out_hbm.at[:, t, pl.ds(c * part, part)]

    def row_source(e, t):
        return stem_at(e, t) if e < CHUNKS else turned.at[0, both, t] if e == CHUNKS else result.at[:, t]

    def row_target(e, t):
        return arrived.at[e, both, t] if e < CHUNKS else swapped.at[both, t] if e == CHUNKS else out_at(t, 1)

    def row_send(e, t):
        remote(row_source(e, t), row_target(e, me), as_sem.at[e], ar_sem.at[e], {"inner": t}).start()

    def send_far(e, planes):
        for h in planes:
            there = jnp.where(z < nz // 2, nz // 2 + h, nz // 2 - 1 - h) * plane

            @pl.loop(0, plane)
            def _(i):
                row_send(e, there + lax.rem(me + i, plane))

    def send_near(e):
        @pl.loop(1, half_n)
        def _(i):
            row_send(e, own_base + lax.rem(me + i, half_n))

    def rows_of(e):
        if e < CHUNKS:
            return arrived.at[e, both, pl.ds(0, n - 1)]
        if e == CHUNKS:
            return swapped.at[both, pl.ds(0, n - 1)]
        return out_hbm.at[:, pl.ds(0, n - 1), pl.ds(part, part)]

    def row_wait(e):
        part_rows = rows_of(e)
        return remote(part_rows, part_rows, as_sem.at[e], ar_sem.at[e], core_peer)

    def build_onehot(s):
        @pl.loop(0, total // LANES)
        def _(i):
            span = pl.ds(pl.multiple_of(i * LANES, LANES), LANES)
            target = lax.broadcasted_iota(jnp.int32, (LANES, total), 0) + i * LANES
            onehot[span, :] = jnp.where(order[s : s + 1, :] == target, 1.0, 0.0).astype(BF16)

    def prepare(s, first=0, last=None):
        @pl.loop(first, columns // TILE if last is None else last)
        def _(j):
            cols = pl.ds(pl.multiple_of(j * TILE, TILE), TILE)
            for p in range(2):
                block_rows = gathered[s, :, p, :, cols].reshape(total, TILE)
                for i in range(total // TILE):
                    span = slice(i * TILE, (i + 1) * TILE)
                    weights[s, p, span, cols] = jnp.dot(
                        onehot[span, :], block_rows, preferred_element_type=F32
                    ).astype(BF16)

    def negate(left):
        @pl.loop(0, n)
        def _(g):
            left[0, g] = -left[2, g]

    def multiply(s, left, store):
        @pl.loop(0, columns // TILE)
        def _(j):
            cols = pl.ds(pl.multiple_of(j * TILE, TILE), TILE)
            straight = left[1:3].reshape(2 * rows, total)
            crossed = left[0:2].reshape(2 * rows, total)
            product = jnp.dot(straight, weights[s, 0, :, cols], preferred_element_type=F32) + jnp.dot(
                crossed, weights[s, 1, :, cols], preferred_element_type=F32
            )
            store(j, cols, product[:rows], product[rows:])

    low_half = lax.broadcasted_iota(jnp.int32, (part, LANES), 1) < LANES // 2

    def turn(into):
        def store(j, cols, real, imag):
            for p, value in ((1, real), (2, imag)):
                for t in range(TILE // LANES):
                    d = (j * (TILE // LANES) + t) * 2
                    lanes = slice(t * LANES, (t + 1) * LANES)
                    for h in range(n // 2):
                        first = value[2 * h * part : (2 * h + 1) * part, lanes]
                        second = value[(2 * h + 1) * part : (2 * h + 2) * part, lanes]
                        mixed = pltpu.roll(jnp.where(low_half, second, first), LANES // 2, 1)
                        at = slice(h * LANES, (h + 1) * LANES)
                        for b, block_value in ((d, jnp.where(low_half, first, mixed)), (d + 1, jnp.where(low_half, mixed, second))):
                            into[p, b, :, at] = block_value.astype(BF16)
                            if p == 2:
                                into[0, b, :, at] = (-block_value).astype(BF16)
        return store

    def keep(into):
        def store(j, cols, real, imag):
            into[0, :, :, cols] = real.astype(BF16).reshape(n, part, TILE)
            into[1, :, :, cols] = imag.astype(BF16).reshape(n, part, TILE)
        return store

    tiles = columns // TILE
    outward = tuple(range(nz // 2))
    branches_in[0].wait()
    begin_z(0)
    greet(meet_sem.at[0])
    branches_in[1].wait()
    begin_z(1)
    begin_side(0)
    begin_side(1)
    order_in.wait()
    build_onehot(0)
    z_step(0, 1)
    side_send(0, 1)
    meet(0)
    branches_in[2].wait()
    begin_z(2)
    z_step(1, 1)
    side_send(1, 1)
    meet(1)
    side_step(0, 0)
    z_step(0, 2)
    side_send(0, 2)
    meet(2)
    z_step(2, 1)
    z_step(1, 2)
    side_send(1, 2)
    meet(3)
    send_far(0, outward)
    side_step(0, 1)
    z_step(0, 3)
    side_send(0, 3)
    side_step(1, 0)
    side_step(0, 2)
    diagonal_step(0, 0)
    z_step(1, 3)
    side_send(1, 3)
    side_step(1, 1)
    send_near(0)
    z_step(2, 2)
    side_step(0, 3)
    diagonal_step(0, 1)
    side_step(1, 2)
    diagonal_step(0, 2)
    send_far(1, outward[::-1])
    side_step(1, 3)
    diagonal_step(0, 3)
    send_near(1)
    begin_side(2)
    side_send(2, 1)
    side_send(2, 2)
    finish(0)
    prepare(0, 0, tiles // 2)
    diagonal_step(1, 0)
    diagonal_step(1, 1)
    prepare(0, tiles // 2, tiles)
    diagonal_step(1, 2)
    diagonal_step(1, 3)
    build_onehot(1)
    finish(1)
    prepare(1, 0, tiles // 2)
    side_step(2, 0)
    z_step(2, 3)
    side_send(2, 3)
    prepare(1, tiles // 2, tiles)
    stem_in[0].wait()
    row_wait(0).wait_recv()
    negate(arrived.at[0])
    multiply(0, arrived.at[0], turn(middle))
    diagonal_step(2, 0)
    multiply(1, middle, turn(turned.at[0]))
    swapped[both, me] = turned[0, both, me]
    send_far(2, outward[:1])
    build_onehot(2)
    side_step(2, 1)
    side_step(2, 2)
    side_step(2, 3)
    stem_in[1].wait()
    row_wait(1).wait_recv()
    send_far(2, outward[1:])
    send_near(2)
    negate(arrived.at[1])
    multiply(0, arrived.at[1], turn(middle))
    multiply(1, middle, turn(turned.at[1]))
    diagonal_step(2, 1)
    diagonal_step(2, 2)
    diagonal_step(2, 3)
    finish(2)
    prepare(2)
    multiply(2, turned.at[1], keep(result))
    send_far(3, outward[::-1])
    send_near(3)
    own_out = pltpu.make_async_copy(result.at[:, me], out_at(me, 1), here_sem.at[0])
    own_out.start()
    row_wait(2).wait_recv()
    negate(swapped)
    multiply(2, swapped, keep(final))
    first_out = pltpu.make_async_copy(final, out_hbm.at[:, :, pl.ds(0, part)], out_sem)
    first_out.start()

    for s in range(sections):
        for t in range(nz - 1):
            for way in (0, 1):
                @pl.when(z_sends(t, way))
                def _():
                    z_copy(s, t, way).wait_send()
        for zz in range(nz):
            @pl.when(z != zz)
            def _():
                x_copy(s, zz).wait_send()

            y_copy(s, zz).wait_send()
            diagonal_y(s, zz).wait_send()
        half = gathered.at[s, pl.ds(0, n // CORES)]
        remote(half, half, cs_sem.at[s], cr_sem.at[s], core_peer).wait_send()
    for e in range(2 * CHUNKS):
        row_wait(e).wait_send()
    own_out.wait()
    first_out.wait()
    row_wait(3).wait_recv()


def fused(n, stem_slab, branches, column_order):
    sections, _, depth, columns = branches.shape
    share = stem_slab.shape[1] // n
    part = share // CHUNKS
    nz = n // (CORES * YS)
    total = n * depth
    dma = pltpu.SemaphoreType.DMA
    stem = stem_slab.reshape(2, n, share, columns)
    result = pl.pallas_call(
        functools.partial(kernel, n),
        out_shape=pltpu.VMEM(stem.shape, BF16),
        in_specs=[pl.BlockSpec(memory_space=pltpu.HBM)] * 3,
        out_specs=pl.BlockSpec(memory_space=pl.ANY),
        scratch_shapes=[
            pltpu.VMEM(branches.shape, BF16),
            pltpu.VMEM(column_order.shape, jnp.int32),
            pltpu.VMEM((sections, n, 2, depth, columns), BF16),
            pltpu.VMEM((total, total), BF16),
            pltpu.VMEM((sections, 2, total, columns), BF16),
            pltpu.VMEM((CHUNKS, 3, n, part, columns), BF16),
            pltpu.VMEM((3, n, part, columns), BF16),
            pltpu.VMEM((CHUNKS, 3, n, part, columns), BF16),
            pltpu.VMEM((3, n, part, columns), BF16),
            pltpu.VMEM((2, n, part, columns), BF16),
            pltpu.VMEM((2, n, part, columns), BF16),
            dma((sections,)),
            dma((sections, nz, 2)),
            dma((sections, nz, 2)),
            *[dma((sections, nz))] * 6,
            dma((sections,)),
            dma((sections,)),
            dma((2 * CHUNKS,)),
            dma((2 * CHUNKS,)),
            dma((CHUNKS,)),
            dma,
            dma((sections,)),
            dma,
            pltpu.SemaphoreType.REGULAR((nz,)),
        ],
        compiler_params=pltpu.CompilerParams(
            collective_id=0, has_side_effects=True, vmem_limit_bytes=61 * 2**20
        ),
    )(stem, branches, column_order)
    return result.reshape(stem_slab.shape)


def solution(mesh):
    n = mesh.shape["inner"]

    def local(stem_slab, branches, column_order):
        columns = branches.shape[3]
        fits = mesh.shape["parts"] == 2 and 2 * (columns // n) == LANES and n == 4 * CORES * YS
        even = stem_slab.shape[1] == n * CHUNKS * PACK and columns % TILE == 0
        if fits and even and branches.shape[0] == 3 and columns == n * branches.shape[2]:
            return fused(n, stem_slab, branches, column_order)
        return plain(stem_slab, branches, column_order)

    in_specs = (P(None, ("parts", "inner"), None), P(None, None, "inner", None), P())
    out_specs = P(None, ("parts", "inner"), None)
    return jax.shard_map(local, mesh=mesh, in_specs=in_specs, out_specs=out_specs, check_vma=False)
```
